32 devices in a mesh: dp: 1, sp: 32 (over x, y, z, core).
Axes of the slice: x: 2, y: 2, z: 4, core: 2. Of those that a mesh axis runs over, the one named last changes fastest.
Arguments:
- q: bfloat16 [32, 32, 96], P('dp')
- k: bfloat16 [32, 8192, 32, 96], P('dp', 'sp')
- v: bfloat16 [32, 8192, 32, 96], P('dp', 'sp')
Outputs:
- q: bfloat16 [32, 32, 96], P('dp')
All inputs are finite; a program needn't handle non-finite values.
Results may differ from the reference program's by a relative error of at most 0.012.
Values are sent between devices in bfloat16 or wider.
A program may use at most 2 GiB of HBM per device.

```python
import jax
import jax.numpy as jnp

BATCH = 32
CACHE = 8192
HEADS = 32
KV_HEADS = 32
HEAD = 96


def setup_inputs(seed: int = 0, part: int = 0) -> dict:
    kq, kk, kv = (jax.random.fold_in(k, part) for k in jax.random.split(jax.random.key(seed), 3))
    return {
        "q": (3 * jax.random.normal(kq, (BATCH, HEADS, HEAD), jnp.float32)).astype(jnp.bfloat16),
        "k": jax.random.normal(kk, (BATCH, CACHE, KV_HEADS, HEAD), jnp.float32).astype(jnp.bfloat16),
        "v": jax.random.normal(kv, (BATCH, CACHE, KV_HEADS, HEAD), jnp.float32).astype(jnp.bfloat16),
    }


def einsum(form, a, b):
    return jnp.einsum(form, a.astype(jnp.float32), b.astype(jnp.float32))


def reference(q, k, v):
    grouped = q.reshape(BATCH, KV_HEADS, -1, HEAD)
    scores = einsum("bgsd,bugd->bgsu", grouped, k) * HEAD**-0.5
    weights = jax.nn.softmax(scores, -1).astype(jnp.bfloat16)
    return einsum("bgsu,bugd->bgsd", weights, v).astype(jnp.bfloat16).reshape(BATCH, HEADS, HEAD)
```

```python
import functools

import jax
import jax.numpy as jnp
from jax import lax
from jax.experimental import pallas as pl
from jax.experimental.pallas import tpu as pltpu
from jax.sharding import PartitionSpec as P

SLOTS = 4
HALF = 16
LANES = 128


def partner(me, step, n):
    mask, out, bit = n - 1 - step, 0, 1
    while bit < n:
        out = out + ((me // bit + mask // bit) % 2) * bit
        bit *= 2
    return out


def iotas(rows):
    shape = (rows, LANES)
    return lax.broadcasted_iota(jnp.int32, shape, 0), lax.broadcasted_iota(jnp.int32, shape, 1)


def rolled(x, shifts):
    quarter = iotas(x.shape[0])[0] % 4
    out = x
    for m in range(1, 4):
        out = jnp.where(quarter == m, pltpu.roll(x, shifts[m], 1), out)
    return out


def spread(q, head):
    row, lane = iotas(HALF)
    turned = rolled(q, (0, 96, 64, 32))
    tiles = []
    for g in range(HALF // 4):
        for t in range(3):
            at = LANES * t + lane - head * (row % 4)
            keep = (row // 4 == g) & (at >= 0) & (at < head)
            tiles.append(jnp.where(keep, turned, 0.0).astype(jnp.bfloat16))
    return jnp.concatenate(tiles, 1)


def diagonal(o):
    row, lane = iotas(8)
    m = row % 4
    out = []
    for r in range(HALF // 8):
        a, b, c = (
            jnp.where(row < 4, o[8 * r : 8 * r + 8, LANES * (6 * r + t) :][:, :LANES], o[8 * r : 8 * r + 8, LANES * (6 * r + 3 + t) :][:, :LANES])
            for t in range(3)
        )
        first = (m == 0) | ((m == 1) & (lane >= 96))
        second = (m == 1) | ((m == 2) & (lane >= 64))
        out.append(jnp.where(first, a, jnp.where(second, b, c)))
    return rolled(jnp.concatenate(out, 0), (0, 32, 64, 96))


def kernel(n, axes, q_ref, k_hbm, v_hbm, out_ref, kbuf, vbuf, qpad, parts, recv, done, ksem, vsem, send_sem, recv_sem, out_send, out_recv):
    heads, head = q_ref.shape[1], q_ref.shape[2]
    rows = HALF * head
    scale = head**-0.5
    me = lax.axis_index(axes)

    def device(i):
        return {axes: i}

    def k_copy(s):
        return pltpu.make_async_copy(k_hbm.at[partner(me, s, n)], kbuf.at[s % SLOTS], ksem.at[s % SLOTS])

    def v_copy(s):
        return pltpu.make_async_copy(v_hbm.at[partner(me, s, n)], vbuf.at[s % SLOTS], vsem.at[s % SLOTS])

    for s in range(SLOTS):
        k_copy(s).start()
        if s < SLOTS - 1:
            v_copy(s).start()

    barrier = pltpu.get_barrier_semaphore()

    def greet(s, c):
        pl.semaphore_signal(barrier, inc=1, device_id=device(partner(me, s, n)), device_id_type=pl.DeviceIdType.MESH)
        return c

    lax.fori_loop(0, n - 1, greet, 0)
    qpad[...] = jnp.zeros_like(qpad)

    def scores(s):
        qpad[:, :head] = q_ref[partner(me, s, n)].astype(jnp.float32)
        out = []
        for i in range(heads // HALF):
            qd = spread(qpad[HALF * i : HALF * (i + 1)], head)
            out.append(jnp.dot(qd, kbuf[s % SLOTS, rows * i : rows * (i + 1)], preferred_element_type=jnp.float32))
        x = jnp.concatenate(out, 0) * scale
        high = jnp.max(x, -1, keepdims=True)
        w = jnp.exp(x - high)
        return w.astype(jnp.bfloat16), jnp.sum(w, -1, keepdims=True), high

    def part(s, w, total, high):
        seen = []
        for i in range(heads // HALF):
            o = lax.dot_general(
                w[HALF * i : HALF * (i + 1)],
                vbuf[s % SLOTS, rows * i : rows * (i + 1)],
                (((1,), (1,)), ((), ())),
                preferred_element_type=jnp.float32,
            )
            seen.append(diagonal(o))
        lane = iotas(heads)[1]
        return jnp.where(lane < head, jnp.concatenate(seen, 0), jnp.where(lane == head, total, high))

    def part_copy(s):
        to = partner(me, s, n)
        return pltpu.make_async_remote_copy(
            src_ref=parts.at[s],
            dst_ref=recv.at[s],
            send_sem=send_sem.at[s],
            recv_sem=recv_sem.at[s],
            device_id=device(to),
            device_id_type=pl.DeviceIdType.MESH,
        )

    def out_copy(s):
        to = partner(me, s, n)
        return pltpu.make_async_remote_copy(
            src_ref=done,
            dst_ref=out_ref.at[me],
            send_sem=out_send.at[s],
            recv_sem=out_recv.at[s],
            device_id=device(to),
            device_id_type=pl.DeviceIdType.MESH,
        )

    k_copy(0).wait()
    first = scores(0)
    pl.semaphore_wait(barrier, n - 1)

    def body(s, carry):
        @pl.when((s >= 1) & (s + SLOTS - 1 < n))
        def _():
            k_copy(s + SLOTS - 1).start()

        @pl.when(s + SLOTS - 1 < n)
        def _():
            v_copy(s + SLOTS - 1).start()

        v_copy(s).wait()
        k_copy(s + 1).wait()
        parts[s] = part(s, *carry)
        after = scores(s + 1)
        part_copy(s).start()
        return after

    last = lax.fori_loop(0, n - 1, body, first)
    v_copy(n - 1).wait()
    recv[n - 1] = part(n - 1, *last)

    def arrived(s, c):
        part_copy(s).wait_recv()
        return c

    lax.fori_loop(0, n - 1, arrived, 0)
    lane = iotas(heads)[1]

    def highest(s, top):
        return jnp.maximum(top, recv[s])

    top = recv[0]
    for s in range(1, n):
        top = jnp.maximum(top, recv[s])
    top = top[:, head + 1 : head + 2]
    acc = jnp.zeros((heads, LANES), jnp.float32)
    for s in range(n):
        x = recv[s]
        acc = acc + x * jnp.exp(x[:, head + 1 : head + 2] - top)
    result = (acc / acc[:, head : head + 1])[:, :head].astype(jnp.bfloat16)
    done[...] = result
    out_ref[me] = result

    def tell(s, c):
        out_copy(s).start()
        return c

    lax.fori_loop(0, n - 1, tell, 0)

    def finish(s, c):
        part_copy(s).wait_send()
        out_copy(s).wait()
        return c

    lax.fori_loop(0, n - 1, finish, 0)


def solution(mesh):
    n = mesh.shape["sp"]

    def step(q, k, v):
        batch, tokens, heads, head = k.shape
        k, v = (x.transpose(0, 2, 3, 1).reshape(batch, heads * head, tokens) for x in (k, v))
        dma = pltpu.SemaphoreType.DMA
        return pl.pallas_call(
            functools.partial(kernel, n, "sp"),
            out_shape=jax.ShapeDtypeStruct(q.shape, jnp.bfloat16),
            in_specs=[pl.BlockSpec(memory_space=pltpu.VMEM), pl.BlockSpec(memory_space=pl.ANY), pl.BlockSpec(memory_space=pl.ANY)],
            out_specs=pl.BlockSpec(memory_space=pltpu.VMEM),
            scratch_shapes=[
                pltpu.VMEM((SLOTS, heads * head, tokens), jnp.bfloat16),
                pltpu.VMEM((SLOTS, heads * head, tokens), jnp.bfloat16),
                pltpu.VMEM((heads, LANES), jnp.float32),
                pltpu.VMEM((n, heads, LANES), jnp.float32),
                pltpu.VMEM((n, heads, LANES), jnp.float32),
                pltpu.VMEM((heads, head), jnp.bfloat16),
                dma((SLOTS,)),
                dma((SLOTS,)),
                dma((n,)),
                dma((n,)),
                dma((n,)),
                dma((n,)),
            ],
            compiler_params=pltpu.CompilerParams(collective_id=0, has_side_effects=True, vmem_limit_bytes=60 * 2**20),
        )(q, k, v)

    return jax.shard_map(
        step,
        mesh=mesh,
        in_specs=(P("dp", None, None), P("dp", "sp", None, None), P("dp", "sp", None, None)),
        out_specs=P("dp", None, None),
        check_vma=False,
    )
```

```python
import functools

import jax
import jax.numpy as jnp
from jax import lax
from jax.experimental import pallas as pl
from jax.experimental.pallas import tpu as pltpu
from jax.sharding import PartitionSpec as P


TURN = 4
HALF = 16
LANES = 128
MESH = pl.DeviceIdType.MESH


def iotas(rows):
    shape = (rows, LANES)
    return lax.broadcasted_iota(jnp.int32, shape, 0), lax.broadcasted_iota(jnp.int32, shape, 1)


def rolled(x, shifts):
    quarter = iotas(x.shape[0])[0] % 4
    out = x
    for m in range(1, 4):
        out = jnp.where(quarter == m, pltpu.roll(x, shifts[m], 1), out)
    return out


def spread(q, head):
    row, lane = iotas(HALF)
    turned = rolled(q, (0, 96, 64, 32))
    tiles = []
    for g in range(HALF // 4):
        for t in range(3):
            at = LANES * t + lane - head * (row % 4)
            keep = (row // 4 == g) & (at >= 0) & (at < head)
            tiles.append(jnp.where(keep, turned, 0.0).astype(jnp.bfloat16))
    return jnp.concatenate(tiles, 1)


def diagonal(o):
    row, lane = iotas(8)
    m = row % 4
    out = []
    for r in range(HALF // 8):
        a, b, c = (
            jnp.where(row < 4, o[8 * r : 8 * r + 8, LANES * (6 * r + t) :][:, :LANES], o[8 * r : 8 * r + 8, LANES * (6 * r + 3 + t) :][:, :LANES])
            for t in range(3)
        )
        first = (m == 0) | ((m == 1) & (lane >= 96))
        second = (m == 1) | ((m == 2) & (lane >= 64))
        out.append(jnp.where(first, a, jnp.where(second, b, c)))
    return rolled(jnp.concatenate(out, 0), (0, 32, 64, 96))


def kernel(n, axis, q_hbm, k_hbm, v_hbm, out_ref, kbuf, vbuf, qbuf, qpad, parts, recv, done, qsem, ksem, vsem, send_sem, recv_sem, out_send, out_recv):
    heads, head = q_hbm.shape[1], q_hbm.shape[2]
    rows = HALF * head
    scale = head**-0.5
    turns = n // TURN
    me = lax.axis_index(axis)
    bits = n.bit_length() - 1
    low = TURN.bit_length() - 1
    flips = [2**i - 2 ** (i + 1) * lax.rem(lax.div(me, 2**i), 2) for i in range(bits)]

    def peer(mask):
        out = me
        for i in range(bits):
            if mask >> i & 1:
                out = out + flips[i]
        return out

    lows = [peer(TURN - 1 - u) for u in range(TURN)]

    def owner(turn, u):
        if isinstance(turn, int):
            return peer(n - 1 - TURN * turn - u)
        out, mask = lows[u], turns - 1 - turn
        for i in range(low, bits):
            out = out + lax.rem(lax.div(mask, 2 ** (i - low)), 2) * flips[i]
        return out

    def at(turn, u):
        return turn + u // TURN, u % TURN

    def k_copy(turn, u):
        turn, u = at(turn, u)
        return pltpu.make_async_copy(k_hbm.at[owner(turn, u)], kbuf.at[u], ksem.at[u])

    def v_copy(turn, u):
        turn, u = at(turn, u)
        return pltpu.make_async_copy(v_hbm.at[owner(turn, u)], vbuf.at[u], vsem.at[u])

    q_copy = pltpu.make_async_copy(q_hbm, qbuf, qsem)
    k_copy(0, 0).start()
    q_copy.start()
    k_copy(0, 1).start()
    for u in range(TURN):
        v_copy(0, u).start()
        if u + 2 < TURN:
            k_copy(0, u + 2).start()

    barrier = pltpu.get_barrier_semaphore()
    for mask in range(n - 1, 0, -1):
        pl.semaphore_signal(barrier, inc=1, device_id={axis: peer(mask)}, device_id_type=MESH)
    qpad[...] = jnp.zeros_like(qpad)

    def scores(turn, u):
        turn, u = at(turn, u)
        qpad[u, :, :head] = qbuf[owner(turn, u)].astype(jnp.float32)
        out = []
        for i in range(heads // HALF):
            qd = spread(qpad[u, HALF * i : HALF * (i + 1)], head)
            out.append(jnp.dot(qd, kbuf[u, rows * i : rows * (i + 1)], preferred_element_type=jnp.float32))
        return jnp.concatenate(out, 0)

    def weigh(x):
        x = x * scale
        high = jnp.max(x, -1, keepdims=True)
        w = jnp.exp(x - high)
        return w.astype(jnp.bfloat16), jnp.sum(w, -1, keepdims=True), high

    def part(u, w, total, high):
        seen = []
        for i in range(heads // HALF):
            o = lax.dot_general(
                w[HALF * i : HALF * (i + 1)],
                vbuf[u, rows * i : rows * (i + 1)],
                (((1,), (1,)), ((), ())),
                preferred_element_type=jnp.float32,
            )
            seen.append(diagonal(o))
        lane = iotas(heads)[1]
        return jnp.where(lane < head, jnp.concatenate(seen, 0), jnp.where(lane == head, total, high))

    def part_copy(s, to):
        return pltpu.make_async_remote_copy(
            src_ref=parts.at[s], dst_ref=recv.at[s], send_sem=send_sem.at[s], recv_sem=recv_sem.at[s], device_id={axis: to}, device_id_type=MESH
        )

    def out_copy(mask, to=None):
        held = out_ref.at[me if to is None else peer(mask ^ to)]
        return pltpu.make_async_remote_copy(
            src_ref=done if to is None else held,
            dst_ref=held,
            send_sem=out_send.at[mask],
            recv_sem=out_recv.at[mask],
            device_id={axis: peer(mask if to is None else to)},
            device_id_type=MESH,
        )

    q_copy.wait()
    k_copy(0, 0).wait()
    x0 = scores(0, 0)
    k_copy(1, 0).start()
    k_copy(0, 1).wait()
    x1 = scores(0, 1)
    k_copy(1, 1).start()
    pl.semaphore_wait(barrier, n - 1)

    def steps(turn, carry, final):
        weighed, x = carry
        for u in range(TURN):
            s = TURN * turn + u
            v_copy(turn, u).wait()
            if not (final and u + 2 >= TURN):
                k_copy(turn, u + 2).wait()
            p = part(u, *weighed)
            if not (final and u + 1 >= TURN):
                weighed = weigh(x)
            if not (final and u + 2 >= TURN):
                x = scores(turn, u + 2)
            if final and u == TURN - 1:
                recv[s] = p
            else:
                parts[s] = p
                part_copy(s, owner(turn, u)).start()
            if not final:
                v_copy(turn + 1, u).start()
                if not (isinstance(turn, int) and turn == turns - 2 and u + 2 >= TURN):
                    k_copy(turn + 1, u + 2).start()
        return weighed, x

    carry = (weigh(x0), x1)
    carry = lax.fori_loop(0, turns - 2, lambda t, c: steps(t, c, False), carry)
    carry = steps(turns - 2, carry, False)
    steps(turns - 1, carry, True)

    for s in range(n - 1):
        part_copy(s, me).wait_recv()

    top = recv[0]
    for s in range(1, n):
        top = jnp.maximum(top, recv[s])
    top = top[:, head + 1 : head + 2]
    acc = jnp.zeros((heads, LANES), jnp.float32)
    for s in range(n):
        x = recv[s]
        acc = acc + x * jnp.exp(x[:, head + 1 : head + 2] - top)
    result = (acc / acc[:, head : head + 1])[:, :head].astype(jnp.bfloat16)
    done[...] = result
    out_ref[me] = result

    def hops(mask):
        return (mask >> 4 & 1) + (mask >> 3 & 1) + (mask >> 1 & 3)

    away = sorted(range(2, n, 2), key=hops, reverse=True)
    copies = [out_copy(m) for m in [1] + away]
    for c in copies:
        c.start()
    for m in reversed(away):
        out_copy(m).wait_recv()
        copies.append(out_copy(m + 1, 1))
        copies[-1].start()
    for c in copies:
        c.wait_send()
    for m in range(1, n, 2):
        out_copy(m).wait_recv()
    for s in range(n - 1):
        part_copy(s, me).wait_send()


def solution(mesh):
    n = mesh.shape["sp"]

    def step(q, k, v):
        batch, tokens, heads, head = k.shape
        k, v = (x.transpose(0, 2, 3, 1).reshape(batch, heads * head, tokens) for x in (k, v))
        dma = pltpu.SemaphoreType.DMA
        hbm = pl.BlockSpec(memory_space=pltpu.HBM)
        return pl.pallas_call(
            functools.partial(kernel, n, "sp"),
            out_shape=pltpu.VMEM(q.shape, jnp.bfloat16),
            in_specs=[hbm] * 3,
            out_specs=pl.BlockSpec(memory_space=pltpu.VMEM),
            scratch_shapes=[
                pltpu.VMEM((TURN, heads * head, tokens), jnp.bfloat16),
                pltpu.VMEM((TURN, heads * head, tokens), jnp.bfloat16),
                pltpu.VMEM(q.shape, jnp.bfloat16),
                pltpu.VMEM((TURN, heads, LANES), jnp.float32),
                pltpu.VMEM((n, heads, LANES), jnp.float32),
                pltpu.VMEM((n, heads, LANES), jnp.float32),
                pltpu.VMEM((heads, head), jnp.bfloat16),
                dma,
                dma((TURN,)),
                dma((TURN,)),
                dma((n,)),
                dma((n,)),
                dma((n,)),
                dma((n,)),
            ],
            compiler_params=pltpu.CompilerParams(collective_id=0, has_side_effects=True, vmem_limit_bytes=60 * 2**20),
        )(q, k, v)

    return jax.shard_map(
        step,
        mesh=mesh,
        in_specs=(P("dp", None, None), P("dp", "sp", None, None), P("dp", "sp", None, None)),
        out_specs=P("dp", None, None),
        check_vma=False,
    )
```

```python
import functools

import jax
import jax.numpy as jnp
from jax import lax
from jax.experimental import pallas as pl
from jax.experimental.pallas import tpu as pltpu
from jax.sharding import PartitionSpec as P


TURN = 4
HALF = 16
PERM = (0, 3, 1, 2, 4)
ORDER = (3, 2, 1, 0)
EARLY = 24
LANES = 128
MESH = pl.DeviceIdType.MESH


def iotas(rows):
    shape = (rows, LANES)
    return lax.broadcasted_iota(jnp.int32, shape, 0), lax.broadcasted_iota(jnp.int32, shape, 1)


def rolled(x, shifts):
    quarter = iotas(x.shape[0])[0] % 4
    out = x
    for m in range(1, 4):
        out = jnp.where(quarter == m, pltpu.roll(x, shifts[m], 1), out)
    return out


def spread(q, head):
    row, lane = iotas(HALF)
    turned = rolled(q, (0, 96, 64, 32))
    tiles = []
    for g in range(HALF // 4):
        for t in range(3):
            at = LANES * t + lane - head * (row % 4)
            keep = (row // 4 == g) & (at >= 0) & (at < head)
            tiles.append(jnp.where(keep, turned, 0.0).astype(jnp.bfloat16))
    return jnp.concatenate(tiles, 1)


def diagonal(o):
    row, lane = iotas(8)
    m = row % 4
    out = []
    for r in range(o.shape[0] // 8):
        a, b, c = (
            jnp.where(row < 4, o[8 * r : 8 * r + 8, LANES * (6 * r + t) :][:, :LANES], o[8 * r : 8 * r + 8, LANES * (6 * r + 3 + t) :][:, :LANES])
            for t in range(3)
        )
        first = (m == 0) | ((m == 1) & (lane >= 96))
        second = (m == 1) | ((m == 2) & (lane >= 64))
        out.append(jnp.where(first, a, jnp.where(second, b, c)))
    return rolled(jnp.concatenate(out, 0), (0, 32, 64, 96))


def kernel(n, axis, q_hbm, k_hbm, v_hbm, out_ref, kbuf, vbuf, qbuf, qpad, parts, recv, done, qsem, ksem, vsem, lastsem, send_sem, recv_sem, out_send, out_recv):
    heads, head = q_hbm.shape[1], q_hbm.shape[2]
    rows = HALF * head
    scale = head**-0.5
    turns = n // TURN
    me = lax.axis_index(axis)
    bits = n.bit_length() - 1
    low = TURN.bit_length() - 1
    flips = [2**i - 2 ** (i + 1) * lax.rem(lax.div(me, 2**i), 2) for i in range(bits)]

    def peer(mask):
        out = me
        for i in range(bits):
            if mask >> i & 1:
                out = out + flips[i]
        return out

    def flipped(mask):
        return sum((mask >> i & 1) << PERM[i] for i in range(bits))

    lows = [peer(flipped(ORDER[u])) for u in range(TURN)]

    def owner(turn, u):
        if isinstance(turn, int):
            return peer(flipped(TURN * (turns - 1 - turn) + ORDER[u]))
        out, mask = lows[u], turns - 1 - turn
        for i in range(low, bits):
            out = out + lax.rem(lax.div(mask, 2 ** (i - low)), 2) * flips[PERM[i]]
        return out

    def at(turn, u):
        return turn + u // TURN, u % TURN

    def k_copy(turn, u):
        turn, u = at(turn, u)
        return pltpu.make_async_copy(k_hbm.at[owner(turn, u)], kbuf.at[u], ksem.at[u])

    def v_copy(turn, u):
        turn, u = at(turn, u)
        return pltpu.make_async_copy(v_hbm.at[owner(turn, u)], vbuf.at[u], vsem.at[u])

    def last_copies():
        return [
            pltpu.make_async_copy(v_hbm.at[me, pl.ds(rows * i, rows)], vbuf.at[TURN - 1, pl.ds(rows * i, rows)], lastsem.at[i])
            for i in range(heads // HALF)
        ]

    q_copy = pltpu.make_async_copy(q_hbm, qbuf, qsem)
    k_copy(0, 0).start()
    q_copy.start()
    k_copy(0, 1).start()
    for u in range(TURN):
        v_copy(0, u).start()
        if u + 2 < TURN:
            k_copy(0, u + 2).start()

    barrier = pltpu.get_barrier_semaphore()
    for mask in range(n - 1, 0, -1):
        pl.semaphore_signal(barrier, inc=1, device_id={axis: peer(mask)}, device_id_type=MESH)
    qpad[...] = jnp.zeros_like(qpad)

    def scores(turn, u):
        turn, u = at(turn, u)
        qpad[u, :, :head] = qbuf[owner(turn, u)].astype(jnp.float32)
        out = []
        for i in range(heads // HALF):
            qd = spread(qpad[u, HALF * i : HALF * (i + 1)], head)
            out.append(jnp.dot(qd, kbuf[u, rows * i : rows * (i + 1)], preferred_element_type=jnp.float32))
        return jnp.concatenate(out, 0)

    def weigh(x):
        x = x * scale
        high = jnp.max(x, -1, keepdims=True)
        w = jnp.exp(x - high)
        return w.astype(jnp.bfloat16), jnp.sum(w, -1, keepdims=True), high

    def seen(u, i, w):
        return lax.dot_general(
            w[HALF * i : HALF * (i + 1)], vbuf[u, rows * i : rows * (i + 1)], (((1,), (1,)), ((), ())), preferred_element_type=jnp.float32
        )

    def packed(o, total, high):
        lane = iotas(heads)[1]
        return jnp.where(lane < head, jnp.concatenate([diagonal(x) for x in o], 0), jnp.where(lane == head, total, high))

    def part(u, w, total, high):
        return packed([seen(u, i, w) for i in range(heads // HALF)], total, high)

    def part_copy(s, to):
        return pltpu.make_async_remote_copy(
            src_ref=parts.at[s], dst_ref=recv.at[s], send_sem=send_sem.at[s], recv_sem=recv_sem.at[s], device_id={axis: to}, device_id_type=MESH
        )

    def out_copy(mask, to=None, device=None):
        held = out_ref.at[me if to is None else peer(mask ^ to)]
        return pltpu.make_async_remote_copy(
            src_ref=done if to is None else held,
            dst_ref=held,
            send_sem=out_send.at[mask],
            recv_sem=out_recv.at[mask],
            device_id={axis: peer(mask if to is None else to) if device is None else device},
            device_id_type=MESH,
        )

    q_copy.wait()
    k_copy(0, 0).wait()
    x0 = scores(0, 0)
    k_copy(1, 0).start()
    k_copy(0, 1).wait()
    x1 = scores(0, 1)
    k_copy(1, 1).start()
    pl.semaphore_wait(barrier, n - 1)

    def start_all(copies):
        for c in copies:
            c.start()

    def steps(turn, carry):
        weighed, x = carry
        for u in range(TURN):
            s = TURN * turn + u
            v_copy(turn, u).wait()
            k_copy(turn, u + 2).wait()
            p = part(u, *weighed)
            weighed = weigh(x)
            x = scores(turn, u + 2)
            parts[s] = p
            part_copy(s, owner(turn, u)).start()
            if not isinstance(turn, int):
                v_copy(turn + 1, u).start()
                k_copy(turn + 1, u + 2).start()
            elif u < 2:
                v_copy(turn + 1, u).start()
                if u == 1:
                    k_copy(turn + 1, 2).start()
            elif u == 2:
                k_copy(turn + 1, 3).start()
                v_copy(turn + 1, 2).start()
            else:
                start_all(last_copies())
        return weighed, x

    def gather(first, last):
        top = recv[first]
        for s in range(first + 1, last):
            top = jnp.maximum(top, recv[s])
        top = top[:, head + 1 : head + 2]
        acc = jnp.zeros((heads, LANES), jnp.float32)
        for s in range(first, last):
            x = recv[s]
            acc = acc + x * jnp.exp(x[:, head + 1 : head + 2] - top)
        return acc, top

    carry = (weigh(x0), x1)
    carry = lax.fori_loop(0, turns - 2, steps, carry)
    weighed, x = steps(turns - 2, carry)
    final = turns - 1
    for s in range(EARLY):
        part_copy(s, me).wait_recv()
    early, before = gather(0, EARLY)

    def send(s, p):
        parts[s] = p
        part_copy(s, owner(final, s % TURN)).start()

    v_copy(final, 0).wait()
    p, weighed = part(0, *weighed), weigh(x)
    send(n - 4, p)
    v_copy(final, 1).wait()
    send(n - 3, part(1, *weighed))
    k_copy(final, 2).wait()
    x = scores(final, 2)
    k_copy(final, 3).wait()
    weighed, x = weigh(x), scores(final, 3)
    v_copy(final, 2).wait()
    o = [seen(2, i, weighed[0]) for i in range(heads // HALF)]
    own = weigh(x)
    send(n - 2, packed(o, *weighed[1:]))
    halves = last_copies()
    halves[0].wait()
    ends = [seen(3, 0, own[0])]
    halves[1].wait()
    ends.append(seen(3, 1, own[0]))
    recv[n - 1] = packed(ends, *own[1:])
    for s in range(EARLY, n - 1):
        part_copy(s, me).wait_recv()
    late, after = gather(EARLY, n)
    top = jnp.maximum(before, after)
    acc = early * jnp.exp(before - top) + late * jnp.exp(after - top)
    result = (acc / acc[:, head : head + 1])[:, :head].astype(jnp.bfloat16)
    done[...] = result
    out_ref[me] = result

    def hops(mask):
        return (mask >> 4 & 1) + (mask >> 3 & 1) + (mask >> 1 & 3)

    away = sorted(range(2, n, 2), key=hops, reverse=True)
    copies = [out_copy(m) for m in [1] + away]
    home = me - lax.rem(me, 2)
    copies[0].start()

    @pl.when(home != 0)
    def _():
        out_copy(home, None, lax.rem(me, 2)).start()

    for m, c in zip(away, copies[1:]):
        pl.when(home != m)(c.start)
    for m in reversed(away):
        out_copy(m).wait_recv()
        copies.append(out_copy(m + 1, 1))
        copies[-1].start()
    for c in copies:
        c.wait_send()
    for m in range(1, n, 2):
        out_copy(m).wait_recv()
    for s in range(n - 1):
        part_copy(s, me).wait_send()


def solution(mesh):
    n = mesh.shape["sp"]

    def step(q, k, v):
        batch, tokens, heads, head = k.shape
        k, v = (x.transpose(0, 2, 3, 1).reshape(batch, heads * head, tokens) for x in (k, v))
        dma = pltpu.SemaphoreType.DMA
        hbm = pl.BlockSpec(memory_space=pltpu.HBM)
        return pl.pallas_call(
            functools.partial(kernel, n, "sp"),
            out_shape=pltpu.VMEM(q.shape, jnp.bfloat16),
            in_specs=[hbm] * 3,
            out_specs=pl.BlockSpec(memory_space=pltpu.VMEM),
            scratch_shapes=[
                pltpu.VMEM((TURN, heads * head, tokens), jnp.bfloat16),
                pltpu.VMEM((TURN, heads * head, tokens), jnp.bfloat16),
                pltpu.VMEM(q.shape, jnp.bfloat16),
                pltpu.VMEM((TURN, heads, LANES), jnp.float32),
                pltpu.VMEM((n, heads, LANES), jnp.float32),
                pltpu.VMEM((n, heads, LANES), jnp.float32),
                pltpu.VMEM((heads, head), jnp.bfloat16),
                dma,
                dma((TURN,)),
                dma((TURN,)),
                dma((heads // HALF,)),
                dma((n,)),
                dma((n,)),
                dma((n,)),
                dma((n,)),
            ],
            compiler_params=pltpu.CompilerParams(collective_id=0, has_side_effects=True, vmem_limit_bytes=60 * 2**20),
        )(q, k, v)

    return jax.shard_map(
        step,
        mesh=mesh,
        in_specs=(P("dp", None, None), P("dp", "sp", None, None), P("dp", "sp", None, None)),
        out_specs=P("dp", None, None),
        check_vma=False,
    )
```
